32 devices in a mesh: row: 4 (over z), col: 4 (over y, x), grid: 2 (over core).
Axes of the slice: x: 2, y: 2, z: 4, core: 2. Of those that a mesh axis runs over, the one named last changes fastest.
Arguments:
- density: bfloat16 [2, 4, 4, 128, 1024], P(None, 'row', None, 'grid', 'col'), may hold values from -0.01171875 to 0.01171875
- basis_values: bfloat16 [16, 256, 512], P(('row', 'col'), 'grid'), may hold values from -6 to 6
- quad_weight: float32 [16, 256], P(('row', 'col'), 'grid'), may hold values from 0.01 to 0.1
- screen: int32 [16, 256], P(('row', 'col'), 'grid'), may hold values 0 or 1
- tile_list: int32 [16, 4], replicated, may hold values from 0 to 7, as said below
Outputs:
- potential_first: bfloat16 [2, 4, 4, 128, 1024], P(None, 'row', None, 'grid', 'col')
- potential_second: bfloat16 [2, 4, 4, 128, 1024], P(None, 'row', None, 'grid', 'col')
The draws below stay inside these ranges and needn't reach their ends.
Inputs may be any that keep to these rules, and one draw needn't show every extreme that they name: `tile_list`: the 4 tile indices of a batch have distinct remainders modulo 4.
All inputs are finite; a program needn't handle non-finite values. No bound on the sum of `screen` on one device may be relied on, other than what follows from the above.
Results may differ from the reference program's by a relative error of at most 0.014.
Values may be sent and summed in bfloat16 or wider, within the bound.
A program may use at most 64 MiB of HBM per device.

```python
import math
import jax
import jax.numpy as jnp
from jax import lax

TILE = 128
TB = 4
RT = 2
PTS = 256
ROW_GROUPS = 4
NT = 8
BATCHES = 16
N_GRID = 2


def draw_tile_list(key, part):
    residues = NT // RT
    row_keys = jax.random.split(jax.random.fold_in(key, 11), BATCHES)
    picked = jax.vmap(lambda single: jax.random.permutation(single, residues)[:TB])(row_keys)
    multiple = jax.random.randint(jax.random.fold_in(key, 12), (BATCHES, TB), 0, RT)
    return (multiple * residues + picked).astype(jnp.int32)


def plant(result, key, smallest, top_value):
    shape = result.shape
    place = [jax.random.randint(jax.random.fold_in(key, axis), (), 0, shape[axis]) for axis in range(len(shape))]
    result = result.at[tuple(place)].set(smallest)
    longest = shape.index(max(shape))
    place[longest] = (place[longest] + 1) % shape[longest]
    return result.at[tuple(place)].set(top_value)


def levels(own_key, extent, pieces, low, largest):
    def one(dim, shards_of):
        heights = jax.random.uniform(jax.random.fold_in(jax.random.fold_in(own_key, 6), dim), (shards_of,), jnp.float32, low / len(pieces), largest / len(pieces))
        return jnp.repeat(jnp.exp(heights), extent[dim] // shards_of).reshape((-1,) + (1,) * (len(extent) - dim - 1))

    factor_of = one(*pieces[0])
    for cut in pieces[1:]:
        factor_of = factor_of * one(*cut)
    return factor_of


def noise(rng, extent, deviation, most, shards=(), kind=jnp.bfloat16):
    array = jax.random.normal(rng, extent, jnp.float32) * deviation
    if len(shards) > 0:
        array = levels(rng, extent, shards, -0.22, 0.18) * array
    return jnp.clip(array, min=-most, max=most).astype(kind)


def setup_inputs(seed: int = 0) -> dict:
    streams_of = jax.random.split(jax.random.key(seed), 6)
    density = noise(streams_of[0], (RT, ROW_GROUPS, 4, TILE, NT * TILE), ((TB * TILE) ** 2) ** -0.5, 0.01171875, ((1, 4), (3, 2), (4, 4)))
    basis_values = noise(streams_of[1], (BATCHES, PTS, TB * TILE), 1.0, 6.0, ((0, 16), (1, 2)))
    quad_weight = jnp.clip(jnp.exp(math.log(0.1) - 2.3025851 * jax.random.uniform(streams_of[2], (BATCHES, PTS), jnp.float32) ** levels(streams_of[2], (BATCHES, PTS), ((0, 16), (1, 2)), -0.2, 0.2)), 0.01, 0.1)
    screen = plant((jax.random.randint(streams_of[3], (BATCHES, PTS), 0, 4) < 3).astype(jnp.int32), jax.random.fold_in(streams_of[3], 1), 0, 1)
    tile_list = draw_tile_list(jax.random.fold_in(streams_of[5], 71), 0)
    return dict(density=density, basis_values=basis_values, quad_weight=quad_weight, screen=screen, tile_list=tile_list)


MIXING = 0.001

def local_potential(densities):
    total_density = densities[:, 0:1]
    spin_density = densities[:, 1:4]
    first_part = total_density / jnp.sqrt(1.0 + total_density * total_density)
    spin_norm = jnp.sqrt(1.0 + lax.optimization_barrier(jnp.sum(spin_density * spin_density, axis=1, keepdims=True)))
    return jnp.concatenate([first_part, spin_density / spin_norm], axis=1)

def build(density, basis_values, point_weight, tile_list):
    row_tiles, n_row, components, tile_width, width = density.shape
    n_tiles = width // tile_width
    tiles = density.reshape(row_tiles * n_row, components, tile_width, n_tiles, tile_width)
    n_col = basis_values.shape[0] // n_row
    half_points = basis_values.shape[1] // N_GRID
    per_batch = tile_list.shape[1]
    span = per_batch * tile_width

    def batch_potential(batch):
        batch_list = tile_list[batch]
        picked = jnp.take(jnp.take(tiles, batch_list, axis=0), batch_list, axis=3)
        dens_block = picked.transpose(0, 2, 1, 3, 4).reshape(span, components * span)
        samples = basis_values[batch]
        contracted = jnp.dot(samples, dens_block, preferred_element_type=jnp.float32)
        densities = lax.optimization_barrier(jnp.sum(contracted.reshape(-1, components, span) * samples.astype(jnp.float32)[:, None, :], axis=2))
        potential_scale = point_weight[batch][:, None] * local_potential(densities)
        weighted = (samples.astype(jnp.float32)[:, None, :] * potential_scale[:, :, None]).astype(jnp.bfloat16)
        weighted = weighted.reshape(-1, components * span)
        combined = jnp.zeros((span, components * span), jnp.float32)
        for member in range(N_GRID):
            lower = member * half_points
            partial_value = lax.dot_general(samples[lower:lower + half_points], weighted[lower:lower + half_points], (((0,), (0,)), ((), ())), preferred_element_type=jnp.float32)
            combined = combined + partial_value.astype(jnp.bfloat16).astype(jnp.float32)
        return combined

    def column_pass(total, column):

        def row_pass(accum, row_index):
            batch = row_index * n_col + column
            batch_list = tile_list[batch]
            slab = batch_potential(batch).reshape(per_batch, tile_width, components, per_batch, tile_width)
            slab = slab.transpose(0, 3, 2, 1, 4)
            accum = accum.at[batch_list[:, None], :, :, batch_list[None, :], :].add(slab)
            return (accum, None)
        start = jnp.zeros((n_tiles, components, tile_width, n_tiles, tile_width), jnp.float32)
        accum, ignored = lax.scan(row_pass, start, jnp.arange(n_row, dtype=jnp.int32))
        return (total + accum.astype(jnp.bfloat16).astype(jnp.float32), None)
    total_start = jnp.zeros((n_tiles, components, tile_width, n_tiles, tile_width), jnp.float32)
    total, ignored = lax.scan(column_pass, total_start, jnp.arange(n_col, dtype=jnp.int32))
    return total.astype(jnp.bfloat16).reshape(row_tiles, n_row, components, tile_width, width)

def reference(density, basis_values, quad_weight, screen, tile_list):
    point_weight = quad_weight * screen.astype(jnp.float32)
    potential_first = build(density, basis_values, point_weight, tile_list)
    updated = (density.astype(jnp.float32) + MIXING * potential_first.astype(jnp.float32)).astype(jnp.bfloat16)
    potential_second = build(updated, basis_values, point_weight, tile_list)
    return (potential_first, potential_second)
```

```python
import functools

import jax
import jax.numpy as jnp
from jax import lax
from jax.experimental import pallas as pl
from jax.experimental.pallas import tpu as pltpu
from jax.sharding import PartitionSpec as P

MIXING = 0.001
AXES = ("row", "col", "grid")


def tile_rows(density_ref, comp):
    return jnp.concatenate([density_ref[k, comp] for k in range(density_ref.shape[0])], axis=0)


def density_kernel(rows_ref, cols_ref, density_ref, out_ref, flipped):
    components = density_ref.shape[1]
    slabs, _, points = rows_ref.shape

    @pl.when(pl.program_id(0) == 0)
    def _():
        for comp in range(components):
            block = tile_rows(density_ref, comp).astype(jnp.float32)
            flipped[comp] = block.T.astype(jnp.bfloat16)

    for slab in range(0, slabs, 2):
        rows = jnp.concatenate([rows_ref[slab], rows_ref[slab + 1]], axis=1)
        cols = jnp.concatenate([cols_ref[slab], cols_ref[slab + 1]], axis=1).astype(jnp.float32)
        for comp in range(components):
            contracted = jnp.dot(flipped[comp], rows, preferred_element_type=jnp.float32)
            total = jnp.sum(contracted * cols, axis=0, keepdims=True)
            out_ref[slab, comp : comp + 1, :] = total[:, :points]
            out_ref[slab + 1, comp : comp + 1, :] = total[:, points:]


def potential_kernel(rows_ref, cols_ref, dens_ref, weight_ref, density_ref, out_ref, updated_ref, total):
    row_tiles, components, half_tile, _ = density_ref.shape
    slabs = rows_ref.shape[0]

    @pl.when(pl.program_id(0) == 0)
    def _():
        total[...] = jnp.zeros_like(total)

    rows_wide = [rows_ref[slab].astype(jnp.float32) for slab in range(slabs)]
    cols = jnp.concatenate([cols_ref[slab] for slab in range(slabs)], axis=1)
    dens = dens_ref[...]
    first = dens[:, 0:1, :]
    spin = dens[:, 1:, :]
    spin_norm = jnp.sqrt(1.0 + jnp.sum(spin * spin, axis=1, keepdims=True))
    weight = weight_ref[...]
    scales = [weight * (first / jnp.sqrt(1.0 + first * first))]
    scales += [weight * (dens[:, comp : comp + 1, :] / spin_norm) for comp in range(1, components)]
    for comp in range(components):
        weighted = jnp.concatenate(
            [(rows_wide[slab] * scales[comp][slab]).astype(jnp.bfloat16) for slab in range(slabs)], axis=1
        )
        total[comp] += lax.dot_general(
            weighted, cols, (((1,), (1,)), ((), ())), preferred_element_type=jnp.float32
        )

    @pl.when(pl.program_id(0) == pl.num_programs(0) - 1)
    def _():
        for comp in range(components):
            rounded = total[comp].astype(jnp.bfloat16)
            for k in range(row_tiles):
                piece = rounded[k * half_tile : (k + 1) * half_tile]
                out_ref[k, comp] = piece
                updated_ref[k, comp] = (
                    density_ref[k, comp].astype(jnp.float32) + MIXING * piece.astype(jnp.float32)
                ).astype(jnp.bfloat16)


def chunk_of(slabs):
    return 8 if slabs % 8 == 0 else 2


def local_densities(rows, cols, density):
    slabs, height, points = rows.shape
    width = cols.shape[1]
    components = density.shape[1]
    chunk = chunk_of(slabs)
    return pl.pallas_call(
        density_kernel,
        grid=(slabs // chunk,),
        out_shape=jax.ShapeDtypeStruct((slabs, components, points), jnp.float32),
        in_specs=[
            pl.BlockSpec((chunk, height, points), lambda i: (i, 0, 0)),
            pl.BlockSpec((chunk, width, points), lambda i: (i, 0, 0)),
            pl.BlockSpec(density.shape, lambda i: (0, 0, 0, 0)),
        ],
        out_specs=pl.BlockSpec((chunk, components, points), lambda i: (i, 0, 0)),
        scratch_shapes=[pltpu.VMEM((components, width, height), jnp.bfloat16)],
    )(rows, cols, density)


def local_potential(rows, cols, dens, weight, density):
    slabs, height, points = rows.shape
    width = cols.shape[1]
    components = density.shape[1]
    chunk = chunk_of(slabs)
    whole = pl.BlockSpec(density.shape, lambda i: (0, 0, 0, 0))
    shape = jax.ShapeDtypeStruct(density.shape, density.dtype)
    return pl.pallas_call(
        potential_kernel,
        grid=(slabs // chunk,),
        out_shape=(shape, shape),
        in_specs=[
            pl.BlockSpec((chunk, height, points), lambda i: (i, 0, 0)),
            pl.BlockSpec((chunk, width, points), lambda i: (i, 0, 0)),
            pl.BlockSpec((chunk, components, points), lambda i: (i, 0, 0)),
            pl.BlockSpec((chunk, 1, points), lambda i: (i, 0, 0)),
            whole,
        ],
        out_specs=(whole, whole),
        scratch_shapes=[pltpu.VMEM((components, height, width), jnp.float32)],
    )(rows, cols, dens, weight, density)


def body(density, basis_values, quad_weight, screen, tile_list):
    n_row = lax.axis_size("row")
    n_grid = lax.axis_size("grid")
    my_row = lax.axis_index("row")
    my_col = lax.axis_index("col")
    my_grid = lax.axis_index("grid")
    density = density[:, 0]
    row_tiles, components, half_tile, width = density.shape
    tile_width = half_tile * n_grid
    own_tiles = width // tile_width
    batches, per_batch = tile_list.shape
    points = basis_values.shape[1]
    slabs = batches * n_grid

    turned = basis_values[0].T
    gathered = lax.all_gather(turned, AXES, axis=0, tiled=False)
    weight = quad_weight[0] * screen[0].astype(jnp.float32)
    weight = lax.all_gather(weight, AXES, axis=0, tiled=False)[:, None, :]

    lists = jnp.repeat(tile_list, n_grid, axis=0)
    split = gathered.reshape(slabs, per_batch, tile_width, points)
    half = lax.dynamic_slice_in_dim(split, my_grid * half_tile, half_tile, axis=2)

    def pick(source, wanted):
        result = jnp.zeros((slabs,) + source.shape[2:], source.dtype)
        for place in range(per_batch):
            match = (lists[:, place] == wanted)[:, None, None]
            result = jnp.where(match, source[:, place], result)
        return result

    rows = jnp.concatenate([pick(half, k * n_row + my_row) for k in range(row_tiles)], axis=1)
    cols = jnp.concatenate([pick(split, my_col * own_tiles + j) for j in range(own_tiles)], axis=1)

    dens = lax.psum(local_densities(rows, cols, density), AXES)
    potential_first, updated = local_potential(rows, cols, dens, weight, density)
    dens = lax.psum(local_densities(rows, cols, updated), AXES)
    potential_second, _ = local_potential(rows, cols, dens, weight, updated)
    return (potential_first[:, None], potential_second[:, None])


def solution(mesh):
    in_specs = (
        P(None, "row", None, "grid", "col"),
        P(("row", "col"), "grid", None),
        P(("row", "col"), "grid"),
        P(("row", "col"), "grid"),
        P(),
    )
    out_specs = (P(None, "row", None, "grid", "col"), P(None, "row", None, "grid", "col"))
    return jax.shard_map(body, mesh=mesh, in_specs=in_specs, out_specs=out_specs, check_vma=False)
```
